32 devices in a mesh: tm: 8 (over z, y), space: 4 (over x, core).
Axes of the slice: x: 2, y: 2, z: 4, core: 2. Of those that a mesh axis runs over, the one named last changes fastest.
Arguments:
- source: float32 [8, 32, 128, 128], P('tm', 'space'), may hold values from -8 to 8
- conductivity: float32 [32, 128, 128], P('space'), may hold values from 0.5 to 4
Outputs:
- solution: float32 [8, 32, 128, 128], P('tm', 'space')
- final_defect: float32 [8, 32, 128, 128], P('tm', 'space')
The draws below stay inside these ranges and needn't reach their ends.
All inputs are finite; a program needn't handle non-finite values.
Results may differ from the reference program's by a relative error of at most 0.000034.
Values sent between devices are 32-bit elements; how exact they have to be, the bound alone decides.
A program may use at most 64 MiB of HBM per device.

```python
import math
import jax
import jax.numpy as jnp

NX = 128
NY = 128
NU = 2
NC = 4
NZ = 32
NT = 8


def level_of(rng, extent, split, smallest, high):
    gain, own = 1.0, jax.random.fold_in(rng, 6)
    for position, parts in split:
        draws = jnp.exp(jax.random.uniform(jax.random.fold_in(own, position), (parts,), jnp.float32, smallest / len(split), high / len(split)))
        gain = gain * jnp.repeat(draws, extent[position] // parts).reshape([-1 if axis == position else 1 for axis in range(len(extent))])
    return gain


def normal_values(key, extent, spread, reach, split=(), held_as=jnp.bfloat16):
    drawn = jax.random.normal(key, extent, jnp.float32) * spread
    if len(split) > 0:
        drawn = level_of(key, extent, split, -0.22, 0.18) * drawn
    return jnp.clip(drawn, min=-reach, max=reach).astype(held_as)


def setup_inputs(seed: int = 0) -> dict:
    key_of = jax.random.split(jax.random.key(seed), 3)
    source = normal_values(key_of[0], (NT, NZ, NX, NY), 1.0, 8.0, ((0, 8), (1, 4)), jnp.float32)
    conductivity = jnp.clip(jnp.exp(math.log(4.0) - 2.0794415 * jax.random.uniform(key_of[1], (NZ, NX, NY), jnp.float32) ** level_of(key_of[1], (NZ, NX, NY), ((0, 4),), -0.2, 0.2)), 0.5, 4.0)
    return {"source": source, "conductivity": conductivity}


OMEGA = 0.8
FINE = (1.0, 1.0, 1.0)
COARSE = (0.25, 0.25, 1.0)


def stencil(padded, weights):
    weight_z, weight_x, weight_y = weights
    centre = padded[..., 1:-1, :, :]
    widths = [(0, 0)] * (centre.ndim - 2) + [(1, 1), (1, 1)]
    framed = jnp.pad(centre, widths)
    along_z = 2.0 * centre - padded[..., 2:, :, :] - padded[..., :-2, :, :]
    along_x = 2.0 * centre - framed[..., 2:, 1:-1] - framed[..., :-2, 1:-1]
    along_y = 2.0 * centre - framed[..., 1:-1, 2:] - framed[..., 1:-1, :-2]
    return weight_z * along_z + weight_x * along_x + weight_y * along_y


def defect(current, right_side, earlier, padded, conduct, stretch, weights):
    applied = current + stretch * conduct * stencil(padded, weights)
    return right_side + earlier - applied


def relaxed(current, right_side, earlier, padded, conduct, stretch, weights):
    weight_sum = 2.0 * (weights[0] + weights[1] + weights[2])
    diagonal = 1.0 + stretch * conduct * weight_sum
    return current + OMEGA * defect(current, right_side, earlier, padded, conduct, stretch, weights) / diagonal


def coarsen(values):
    return 0.25 * ((values[..., 0::2, 0::2, :] + values[..., 1::2, 0::2, :]) + (values[..., 0::2, 1::2, :] + values[..., 1::2, 1::2, :]))


def refine(values):
    return jnp.repeat(jnp.repeat(values, 2, axis=-3), 2, axis=-2)


def pad_planes(values):
    return jnp.pad(values, [(0, 0)] * (values.ndim - 3) + [(1, 1), (0, 0), (0, 0)])


def time_before(values):
    return jnp.concatenate([jnp.zeros_like(values[:1]), values[:-1]], 0)


def smooth(current, right_side, conduct, stretch, weights, repeats):
    for turn_index in range(repeats):
        current = relaxed(current, right_side, time_before(current), pad_planes(current), conduct, stretch, weights)
    return current


def level_defect(current, right_side, conduct, stretch, weights):
    return defect(current, right_side, time_before(current), pad_planes(current), conduct, stretch, weights)


def reference(source, conductivity):
    solution = smooth(jnp.zeros_like(source), source, conductivity, 1.0, FINE, NU)
    defect_fine = level_defect(solution, source, conductivity, 1.0, FINE)
    middle_rhs = defect_fine[0::2] + defect_fine[1::2]
    middle = smooth(jnp.zeros_like(middle_rhs), middle_rhs, conductivity, 2.0, FINE, NU)
    middle_defect = level_defect(middle, middle_rhs, conductivity, 2.0, FINE)
    summed = middle_defect[0::2] + middle_defect[1::2]
    coarse_rhs = coarsen(summed)
    coarse_cond = coarsen(conductivity)
    coarse = smooth(jnp.zeros_like(coarse_rhs), coarse_rhs, coarse_cond, 4.0, COARSE, NC)
    middle = middle + jnp.repeat(refine(coarse), 2, axis=0)
    middle = smooth(middle, middle_rhs, conductivity, 2.0, FINE, NU)
    solution = solution + jnp.repeat(middle, 2, axis=0)
    solution = smooth(solution, source, conductivity, 1.0, FINE, NU)
    final_defect = level_defect(solution, source, conductivity, 1.0, FINE)
    return solution, final_defect
```

```python
import functools

import jax
import jax.numpy as jnp
from jax import lax
from jax.experimental import pallas as pl
from jax.experimental.pallas import tpu as pltpu
from jax.sharding import PartitionSpec as P

NU = 2
NC = 4


OMEGA = 0.8
FINE = (1.0, 1.0, 1.0)
COARSE = (0.25, 0.25, 1.0)


def padded_2(shard, sides, width):
    for axis, dim in sides:
        peers, length = (lax.axis_size(axis), shard.shape[dim])
        up = [(i, (i + 1) % peers) for i in range(peers - 1)]
        down = [(j, i) for i, j in up]
        last = lax.slice_in_dim(shard, length - width, length, axis=dim)
        first = lax.slice_in_dim(shard, 0, width, axis=dim)
        before = lax.ppermute(last, axis, up)
        after = lax.ppermute(first, axis, down)
        shard = jnp.concatenate([before, shard, after], axis=dim)
    return shard


def shifted(shard, axis, by):
    peers = lax.axis_size(axis)
    pairs = [(i, i + by) for i in range(peers) if 0 <= i + by < peers]
    return lax.ppermute(shard, axis, pairs)


def swapped(value, axis, bit):
    mask = 2**bit
    pairs = [(source, source ^ mask) for source in range(lax.axis_size(axis))]
    return lax.ppermute(value, axis, pairs)


def stencil(padded, weights):
    weight_z, weight_x, weight_y = weights
    centre = padded[1:-1, :, 1:-1]
    widened = jnp.pad(padded[1:-1], ((0, 0), (1, 1), (0, 0)))
    along_z = 2.0 * centre - padded[2:, :, 1:-1] - padded[:-2, :, 1:-1]
    along_x = 2.0 * centre - widened[:, 2:, 1:-1] - widened[:, :-2, 1:-1]
    along_y = 2.0 * centre - padded[1:-1, :, 2:] - padded[1:-1, :, :-2]
    return weight_z * along_z + weight_x * along_x + weight_y * along_y


def defect(current, right_side, earlier, padded, conduct, stretch, weights):
    applied = current + stretch * conduct * stencil(padded, weights)
    return right_side + earlier - applied


def relaxed(current, right_side, earlier, padded, conduct, stretch, weights):
    weight_sum = 2.0 * (weights[0] + weights[1] + weights[2])
    diagonal = 1.0 + stretch * conduct * weight_sum
    return (
        current
        + OMEGA * defect(current, right_side, earlier, padded, conduct, stretch, weights) / diagonal
    )


def coarsen(values):
    return 0.25 * (
        values[..., 0::2, 0::2, :]
        + values[..., 1::2, 0::2, :]
        + (values[..., 0::2, 1::2, :] + values[..., 1::2, 1::2, :])
    )


def refine(values):
    return jnp.repeat(jnp.repeat(values, 2, axis=-3), 2, axis=-2)


def zero_columns(values):
    return jnp.pad(values, ((0, 0), (0, 0), (1, 1)))


def plane_faces(values):
    return padded_2(values, (("space", 0),), 1)


def coarse_planes_framed(values):
    return padded_2(values, (("space", 0),), 1)


def fine_frame(values):
    return zero_columns(plane_faces(values))


def step_prior(values):
    return shifted(values, "tm", 1)


def pair_prior(values):
    return shifted(values, "tm", 2)


def group_prior(values):
    return shifted(values, "tm", 4)


def smooth(current, right_side, conduct, stretch, weights, repeats, earlier_of, framing):
    for turn_index in range(repeats):
        current = relaxed(
            current, right_side, earlier_of(current), framing(current), conduct, stretch, weights
        )
    return current


def body(source, conductivity):
    right_side = source[0]
    solution = smooth(
        jnp.zeros_like(right_side), right_side, conductivity, 1.0, FINE, NU, step_prior, fine_frame
    )
    defect_fine = defect(
        solution, right_side, step_prior(solution), fine_frame(solution), conductivity, 1.0, FINE
    )
    middle_full = defect_fine + swapped(defect_fine, "tm", 0)
    middle = smooth(
        jnp.zeros_like(middle_full),
        middle_full,
        conductivity,
        2.0,
        FINE,
        NU,
        pair_prior,
        fine_frame,
    )
    middle_defect = defect(
        middle, middle_full, pair_prior(middle), fine_frame(middle), conductivity, 2.0, FINE
    )
    summed = middle_defect + swapped(middle_defect, "tm", 1)
    coarse_rhs = coarsen(summed)
    coarse_cond = coarsen(conductivity)

    def coarse_frame(values):
        return zero_columns(coarse_planes_framed(values))

    coarse = smooth(
        jnp.zeros_like(coarse_rhs),
        coarse_rhs,
        coarse_cond,
        4.0,
        COARSE,
        NC,
        group_prior,
        coarse_frame,
    )
    middle = middle + refine(coarse)
    middle = smooth(middle, middle_full, conductivity, 2.0, FINE, NU, pair_prior, fine_frame)
    solution = solution + middle
    solution = smooth(solution, right_side, conductivity, 1.0, FINE, NU, step_prior, fine_frame)
    final_defect = defect(
        solution, right_side, step_prior(solution), fine_frame(solution), conductivity, 1.0, FINE
    )
    return (solution[None], final_defect[None])


MESH = pl.DeviceIdType.MESH


def snake(index):
    return index + ((index // 2) % 2) * (1 - 2 * (index % 2))


def scaled(weights, stretch):
    return tuple(stretch * weight for weight in weights)


def fits(steps, peers, slabs, planes, rows, lanes):
    block = rows // peers
    return (
        steps == peers
        and peers % 8 == 0
        and peers & (peers - 1) == 0
        and rows % peers == 0
        and block % 8 == 0
        and planes % 2 == 0
        and lanes % 128 == 0
        and peers <= 16
        and slabs > 1
    )


def cycle_kernel(
    peers,
    slabs,
    source,
    source_far,
    conduct,
    out_solution,
    out_defect,
    rhs, rhs1, rhs2, scrap,
    cond, cond2, gain0, gain1, gain2,
    a1, a2, a3, a4, a5, fd,
    m1, m2, m3, m4,
    k1, k2, k3, k4,
    halo_z, halo_x, halo_z2, halo_x2,
    in_send, in_recv, own_sem,
    h_send, h_recv,
    out_send, out_recv, out_own,
):
    planes, rows, lanes = source.shape
    block = rows // peers
    half_planes, half_block = planes // 2, block // 2
    me, slab = lax.axis_index("tm"), lax.axis_index("space")
    mine = snake(me)
    following, preceding = snake((mine + 1) % peers), snake((mine + peers - 1) % peers)
    has_next, has_prev = mine < peers - 1, mine > 0
    has_up, has_down = slab < slabs - 1, slab > 0

    barrier = pltpu.get_barrier_semaphore()
    for k in range(1, peers):
        pl.semaphore_signal(
            barrier, inc=1, device_id={"tm": me ^ k}, device_id_type=MESH
        )

    @pl.when(has_up)
    def _():
        pl.semaphore_signal(barrier, inc=1, device_id={"space": slab + 1}, device_id_type=MESH)

    @pl.when(has_down)
    def _():
        pl.semaphore_signal(barrier, inc=1, device_id={"space": slab - 1}, device_id_type=MESH)

    neighbours = jnp.where(has_up, 1, 0) + jnp.where(has_down, 1, 0)
    pl.semaphore_wait(barrier, peers - 1 + neighbours)

    def rows_of(index):
        return pl.ds(pl.multiple_of(snake(index) * block, 8), block)

    def inward(peer, step, recv):
        return pltpu.make_async_remote_copy(
            src_ref=source.at[:, rows_of(peer), :],
            dst_ref=rhs.at[:, :, step, :],
            send_sem=in_send.at[peer],
            recv_sem=in_recv.at[recv],
            device_id={"tm": peer},
            device_id_type=MESH,
        )

    order = sorted(range(1, peers), reverse=True)
    for k in order:
        inward(me ^ k, me, me).start()
    own = pltpu.make_async_copy(
        source_far.at[:, rows_of(me), :], rhs.at[:, :, me, :], own_sem
    )
    own.start()

    def fill(z, _):
        for x in range(block):
            row = conduct[z, pl.ds(mine * block + x, 1), :]
            value = jnp.broadcast_to(row, (peers, lanes))
            cond[z, x] = value
            gain0[z, x] = OMEGA / (1.0 + value * (2.0 * sum(FINE)))
            gain1[z, x] = OMEGA / (1.0 + value * (4.0 * sum(FINE)))
        return 0

    lax.fori_loop(0, planes, fill, 0)

    def fill2(z, _):
        for x in range(half_block):
            value = 0.25 * (
                (cond[2 * z, 2 * x] + cond[2 * z + 1, 2 * x])
                + (cond[2 * z, 2 * x + 1] + cond[2 * z + 1, 2 * x + 1])
            )
            cond2[z, x] = value
            gain2[z, x] = OMEGA / (1.0 + value * (8.0 * sum(COARSE)))
        return 0

    lax.fori_loop(0, half_planes, fill2, 0)
    for ref in (a1, a2, a3, a4, a5, m1, m2, m3, m4, k1, k2, k3):
        depth, width = ref.shape[0], ref.shape[1]
        face = jnp.zeros((width, peers, lanes), jnp.float32)
        ref[0] = face
        ref[depth - 1] = face
        cell = jnp.zeros((peers, lanes), jnp.float32)

        def edge(z, _):
            ref[z, 0] = cell
            ref[z, width - 1] = cell
            return 0

        lax.fori_loop(1, depth - 1, edge, 0)

    time = lax.broadcasted_iota(jnp.int32, (1, peers, lanes), 1)
    lane = lax.broadcasted_iota(jnp.int32, (1, peers, lanes), 2)
    not_first, not_last = lane > 0, lane < lanes - 1

    def prior(value, shift):
        return jnp.where(time >= shift, pltpu.roll(value, shift, 1), 0.0)

    def with_partner(value, shift):
        even = (time // shift) % 2 == 0
        return value + jnp.where(
            even, pltpu.roll(value, peers - shift, 1), pltpu.roll(value, shift, 1)
        )

    def residual(ref, z, right, conductivity, weights, shift):
        weight_z, weight_x, weight_y = weights
        width = ref.shape[1] - 2
        inner = slice(1, width + 1)
        centre = ref[z + 1, inner]
        along_z = ref[z, inner] + ref[z + 2, inner]
        along_x = ref[z + 1, 0:width] + ref[z + 1, 2 : width + 2]
        along_y = jnp.where(not_first, pltpu.roll(centre, 1, 2), 0.0) + jnp.where(
            not_last, pltpu.roll(centre, lanes - 1, 2), 0.0
        )
        if weight_z == weight_x == weight_y:
            around = weight_z * (6.0 * centre - (along_z + along_x + along_y))
        else:
            around = (2.0 * (weight_z + weight_x + weight_y)) * centre - (
                weight_z * along_z + weight_x * along_x + weight_y * along_y
            )
        return centre, right + prior(centre, shift) - centre - conductivity * around

    def sweep(new, old, right, conductivity, gain, weights, shift):
        width = old.shape[1] - 2

        def plane(z, _):
            centre, left = residual(old, z, right[z], conductivity[z], weights, shift)
            new[z + 1, 1 : width + 1] = centre + gain[z] * left
            return 0

        lax.fori_loop(0, old.shape[0] - 2, plane, 0)

    def defect_into(new, off, old, right, conductivity, weights, shift):
        width = old.shape[1] - 2

        def plane(z, _):
            new[z + off, off : width + off] = residual(
                old, z, right[z], conductivity[z], weights, shift
            )[1]
            return 0

        lax.fori_loop(0, old.shape[0] - 2, plane, 0)

    def bufs(ref):
        if ref.shape[0] == planes + 2:
            return halo_z, halo_x
        return halo_z2, halo_x2

    def faces(ref, stage):
        into_z, into_x = bufs(ref)
        slot = stage_slot[stage]
        depth, width = ref.shape[0] - 2, ref.shape[1] - 2
        inner, deep = pl.ds(1, width), pl.ds(1, depth)

        def copy(src, dst, side, device):
            return pltpu.make_async_remote_copy(
                src_ref=src,
                dst_ref=dst,
                send_sem=h_send.at[stage, side],
                recv_sem=h_recv.at[stage, side],
                device_id=device,
                device_id_type=MESH,
            )

        return (
            (has_up, has_down, copy(ref.at[depth, inner], into_z.at[slot, 0], 0, {"space": slab + 1})),
            (has_down, has_up, copy(ref.at[1, inner], into_z.at[slot, 1], 1, {"space": slab - 1})),
            (has_next, has_prev, copy(ref.at[deep, width], into_x.at[slot, 0], 2, {"tm": following})),
            (has_prev, has_next, copy(ref.at[deep, 1], into_x.at[slot, 1], 3, {"tm": preceding})),
        )

    stage_slot = {0: 0, 1: 1, 2: 2, 3: 3, 4: 0, 5: 1, 6: 2, 7: 4, 8: 5, 9: 6, 10: 7, 11: 8}
    sent = []

    def send(ref, stage):
        for sends, _, copy in faces(ref, stage):
            pl.when(sends)(copy.start)
        sent.append((ref, stage))

    def receive(ref, stage, new, off, conductivity, gain, weights):
        weight_z, weight_x, _ = weights
        into_z, into_x = bufs(ref)
        slot = stage_slot[stage]
        depth, width = ref.shape[0] - 2, ref.shape[1] - 2
        inner, deep = slice(off, off + width), slice(off, off + depth)
        four = faces(ref, stage)

        def scale(*index):
            value = conductivity[index]
            return value if gain is None else value * gain[index]

        for side, z in ((0, 0), (1, depth - 1)):
            _, arrives, copy = four[side]

            @pl.when(arrives)
            def _(copy=copy, side=side, z=z):
                copy.wait_recv()
                new[z + off, inner] += scale(z) * (weight_z * into_z[slot, side])

        for side, x in ((0, 0), (1, width - 1)):
            _, arrives, copy = four[side + 2]

            @pl.when(arrives)
            def _(copy=copy, side=side, x=x):
                copy.wait_recv()
                new[deep, x + off] += scale(slice(None), x) * (weight_x * into_x[slot, side])

    fine, middle, coarse = FINE, scaled(FINE, 2.0), scaled(COARSE, 4.0)

    own.wait()
    for k in order:
        inward(me, me ^ k, me ^ k).wait_recv()

    def first(z, _):
        a1[z + 1, 1 : block + 1] = gain0[z] * rhs[z]
        return 0

    lax.fori_loop(0, planes, first, 0)
    send(a1, 0)
    sweep(a2, a1, rhs, cond, gain0, fine, 1)
    receive(a1, 0, a2, 1, cond, gain0, fine)
    send(a2, 1)
    defect_into(scrap, 0, a2, rhs, cond, fine, 1)
    receive(a2, 1, scrap, 0, cond, None, fine)

    def restrict_time(z, _):
        value = with_partner(scrap[z], 1)
        rhs1[z] = value
        m1[z + 1, 1 : block + 1] = gain1[z] * value
        return 0

    lax.fori_loop(0, planes, restrict_time, 0)
    send(m1, 2)
    sweep(m2, m1, rhs1, cond, gain1, middle, 2)
    receive(m1, 2, m2, 1, cond, gain1, middle)
    send(m2, 3)
    defect_into(scrap, 0, m2, rhs1, cond, middle, 2)
    receive(m2, 3, scrap, 0, cond, None, middle)

    def restrict(z, _):
        for x in range(half_block):
            quad = (scrap[2 * z, 2 * x] + scrap[2 * z + 1, 2 * x]) + (
                scrap[2 * z, 2 * x + 1] + scrap[2 * z + 1, 2 * x + 1]
            )
            value = 0.25 * with_partner(quad[None], 2)[0]
            rhs2[z, x] = value
            k1[z + 1, x + 1] = gain2[z, x] * value
        return 0

    lax.fori_loop(0, half_planes, restrict, 0)
    send(k1, 4)
    sweep(k2, k1, rhs2, cond2, gain2, coarse, 4)
    receive(k1, 4, k2, 1, cond2, gain2, coarse)
    send(k2, 5)
    sweep(k3, k2, rhs2, cond2, gain2, coarse, 4)
    receive(k2, 5, k3, 1, cond2, gain2, coarse)
    send(k3, 6)
    sweep(k4, k3, rhs2, cond2, gain2, coarse, 4)
    receive(k3, 6, k4, 1, cond2, gain2, coarse)

    def prolong(z, _):
        for x in range(half_block):
            value = k4[z + 1, x + 1]
            for dz in range(2):
                for dx in range(2):
                    at = (2 * z + dz + 1, 2 * x + dx + 1)
                    m3[at] = m2[at] + value
        return 0

    lax.fori_loop(0, half_planes, prolong, 0)
    send(m3, 7)
    sweep(m4, m3, rhs1, cond, gain1, middle, 2)
    receive(m3, 7, m4, 1, cond, gain1, middle)
    send(m4, 8)

    def last_middle(z, _):
        centre, left = residual(m4, z, rhs1[z], cond[z], middle, 2)
        inner = slice(1, block + 1)
        a3[z + 1, inner] = a2[z + 1, inner] + (centre + gain1[z] * left)
        return 0

    lax.fori_loop(0, planes, last_middle, 0)
    receive(m4, 8, a3, 1, cond, gain1, middle)
    send(a3, 9)
    sweep(a4, a3, rhs, cond, gain0, fine, 1)
    receive(a3, 9, a4, 1, cond, gain0, fine)
    send(a4, 10)
    sweep(a5, a4, rhs, cond, gain0, fine, 1)
    receive(a4, 10, a5, 1, cond, gain0, fine)
    send(a5, 11)

    def outward(which, src, off, dst, peer, owner):
        inner, deep = pl.ds(off, block), pl.ds(off, planes)
        return pltpu.make_async_remote_copy(
            src_ref=src.at[deep, inner, peer, :],
            dst_ref=dst.at[:, rows_of(owner), :],
            send_sem=out_send.at[which, peer],
            recv_sem=out_recv.at[which, owner],
            device_id={"tm": peer},
            device_id_type=MESH,
        )

    def home(which, src, off, dst):
        return pltpu.make_async_copy(
            src.at[pl.ds(off, planes), pl.ds(off, block), me, :],
            dst.at[:, rows_of(me), :],
            out_own.at[which],
        )

    for k in order:
        outward(0, a5, 1, out_solution, me ^ k, me).start()
    home(0, a5, 1, out_solution).start()
    defect_into(fd, 0, a5, rhs, cond, fine, 1)
    receive(a5, 11, fd, 0, cond, None, fine)
    for k in order:
        outward(1, fd, 0, out_defect, me ^ k, me).start()
    home(1, fd, 0, out_defect).start()

    for ref, stage in sent:
        for sends, _, copy in faces(ref, stage):
            pl.when(sends)(copy.wait_send)
    for k in order:
        inward(me ^ k, me, me).wait_send()
    for which, src, off, dst in ((0, a5, 1, out_solution), (1, fd, 0, out_defect)):
        home(which, src, off, dst).wait()
        for k in order:
            outward(which, src, off, dst, me ^ k, me).wait_send()
            outward(which, src, off, dst, me, me ^ k).wait_recv()


def fused_body(peers, slabs, source, conductivity):
    _, planes, rows, lanes = source.shape
    block = rows // peers

    def field(depth, width):
        return pltpu.VMEM((depth, width, peers, lanes), jnp.float32)

    plain, framed = field(planes, block), field(planes + 2, block + 2)
    small, small_framed = (
        field(planes // 2, block // 2),
        field(planes // 2 + 2, block // 2 + 2),
    )
    dma = pltpu.SemaphoreType.DMA
    vmem, anywhere = pl.BlockSpec(memory_space=pltpu.VMEM), pl.BlockSpec(memory_space=pl.ANY)
    shape = jax.ShapeDtypeStruct((planes, rows, lanes), jnp.float32)

    def faces_of(slots, depth):
        return pltpu.VMEM((slots, 2, depth, peers, lanes), jnp.float32)

    solution, final_defect = pl.pallas_call(
        functools.partial(cycle_kernel, peers, slabs),
        out_shape=(shape, shape),
        in_specs=[vmem, anywhere, vmem],
        out_specs=(anywhere, anywhere),
        scratch_shapes=[
            plain, plain, small, plain,
            plain, small, plain, plain, small,
            framed, framed, framed, framed, framed, plain,
            framed, framed, framed, framed,
            small_framed, small_framed, small_framed, small_framed,
            faces_of(9, block), faces_of(9, planes),
            faces_of(3, block // 2), faces_of(3, planes // 2),
            dma((peers,)), dma((peers,)), dma,
            dma((12, 4)), dma((12, 4)),
            dma((2, peers)), dma((2, peers)), dma((2,)),
        ],
        compiler_params=pltpu.CompilerParams(
            collective_id=0, has_side_effects=True, vmem_limit_bytes=32 * 1024 * 1024
        ),
    )(source[0], source[0], conductivity)
    return (solution[None], final_defect[None])


def solution(mesh):
    peers, slabs = mesh.shape["tm"], mesh.shape["space"]

    def chosen(source, conductivity):
        steps, planes, rows, lanes = source.shape
        if fits(steps * peers, peers, slabs, planes, rows, lanes):
            return fused_body(peers, slabs, source, conductivity)
        return body(source, conductivity)

    return jax.shard_map(
        chosen,
        mesh=mesh,
        in_specs=(P("tm", "space", None, None), P("space", None, None)),
        out_specs=(P("tm", "space", None, None), P("tm", "space", None, None)),
        check_vma=False,
    )
```

```python
import functools

import jax
import jax.numpy as jnp
from jax import lax
from jax.experimental import pallas as pl
from jax.experimental.pallas import tpu as pltpu
from jax.sharding import PartitionSpec as P

NU = 2
NC = 4


OMEGA = 0.8
FINE = (1.0, 1.0, 1.0)
COARSE = (0.25, 0.25, 1.0)


def padded_2(shard, sides, width):
    for axis, dim in sides:
        peers, length = (lax.axis_size(axis), shard.shape[dim])
        up = [(i, (i + 1) % peers) for i in range(peers - 1)]
        down = [(j, i) for i, j in up]
        last = lax.slice_in_dim(shard, length - width, length, axis=dim)
        first = lax.slice_in_dim(shard, 0, width, axis=dim)
        before = lax.ppermute(last, axis, up)
        after = lax.ppermute(first, axis, down)
        shard = jnp.concatenate([before, shard, after], axis=dim)
    return shard


def shifted(shard, axis, by):
    peers = lax.axis_size(axis)
    pairs = [(i, i + by) for i in range(peers) if 0 <= i + by < peers]
    return lax.ppermute(shard, axis, pairs)


def swapped(value, axis, bit):
    mask = 2**bit
    pairs = [(source, source ^ mask) for source in range(lax.axis_size(axis))]
    return lax.ppermute(value, axis, pairs)


def stencil(padded, weights):
    weight_z, weight_x, weight_y = weights
    centre = padded[1:-1, :, 1:-1]
    widened = jnp.pad(padded[1:-1], ((0, 0), (1, 1), (0, 0)))
    along_z = 2.0 * centre - padded[2:, :, 1:-1] - padded[:-2, :, 1:-1]
    along_x = 2.0 * centre - widened[:, 2:, 1:-1] - widened[:, :-2, 1:-1]
    along_y = 2.0 * centre - padded[1:-1, :, 2:] - padded[1:-1, :, :-2]
    return weight_z * along_z + weight_x * along_x + weight_y * along_y


def defect(current, right_side, earlier, padded, conduct, stretch, weights):
    applied = current + stretch * conduct * stencil(padded, weights)
    return right_side + earlier - applied


def relaxed(current, right_side, earlier, padded, conduct, stretch, weights):
    weight_sum = 2.0 * (weights[0] + weights[1] + weights[2])
    diagonal = 1.0 + stretch * conduct * weight_sum
    return (
        current
        + OMEGA * defect(current, right_side, earlier, padded, conduct, stretch, weights) / diagonal
    )


def coarsen(values):
    return 0.25 * (
        values[..., 0::2, 0::2, :]
        + values[..., 1::2, 0::2, :]
        + (values[..., 0::2, 1::2, :] + values[..., 1::2, 1::2, :])
    )


def refine(values):
    return jnp.repeat(jnp.repeat(values, 2, axis=-3), 2, axis=-2)


def zero_columns(values):
    return jnp.pad(values, ((0, 0), (0, 0), (1, 1)))


def plane_faces(values):
    return padded_2(values, (("space", 0),), 1)


def coarse_planes_framed(values):
    return padded_2(values, (("space", 0),), 1)


def fine_frame(values):
    return zero_columns(plane_faces(values))


def step_prior(values):
    return shifted(values, "tm", 1)


def pair_prior(values):
    return shifted(values, "tm", 2)


def group_prior(values):
    return shifted(values, "tm", 4)


def smooth(current, right_side, conduct, stretch, weights, repeats, earlier_of, framing):
    for turn_index in range(repeats):
        current = relaxed(
            current, right_side, earlier_of(current), framing(current), conduct, stretch, weights
        )
    return current


def body(source, conductivity):
    right_side = source[0]
    solution = smooth(
        jnp.zeros_like(right_side), right_side, conductivity, 1.0, FINE, NU, step_prior, fine_frame
    )
    defect_fine = defect(
        solution, right_side, step_prior(solution), fine_frame(solution), conductivity, 1.0, FINE
    )
    middle_full = defect_fine + swapped(defect_fine, "tm", 0)
    middle = smooth(
        jnp.zeros_like(middle_full),
        middle_full,
        conductivity,
        2.0,
        FINE,
        NU,
        pair_prior,
        fine_frame,
    )
    middle_defect = defect(
        middle, middle_full, pair_prior(middle), fine_frame(middle), conductivity, 2.0, FINE
    )
    summed = middle_defect + swapped(middle_defect, "tm", 1)
    coarse_rhs = coarsen(summed)
    coarse_cond = coarsen(conductivity)

    def coarse_frame(values):
        return zero_columns(coarse_planes_framed(values))

    coarse = smooth(
        jnp.zeros_like(coarse_rhs),
        coarse_rhs,
        coarse_cond,
        4.0,
        COARSE,
        NC,
        group_prior,
        coarse_frame,
    )
    middle = middle + refine(coarse)
    middle = smooth(middle, middle_full, conductivity, 2.0, FINE, NU, pair_prior, fine_frame)
    solution = solution + middle
    solution = smooth(solution, right_side, conductivity, 1.0, FINE, NU, step_prior, fine_frame)
    final_defect = defect(
        solution, right_side, step_prior(solution), fine_frame(solution), conductivity, 1.0, FINE
    )
    return (solution[None], final_defect[None])


MESH = pl.DeviceIdType.MESH


def snake(index):
    return index + ((index // 2) % 2) * (1 - 2 * (index % 2))


def scaled(weights, stretch):
    return tuple(stretch * weight for weight in weights)


def fits(steps, peers, slabs, planes, rows, lanes):
    block = rows // peers
    return (
        steps == peers
        and peers % 8 == 0
        and peers & (peers - 1) == 0
        and rows % peers == 0
        and block % 8 == 0
        and planes % 2 == 0
        and lanes % 128 == 0
        and peers <= 16
        and slabs > 1
    )


def cycle_kernel(
    peers,
    slabs,
    source_far,
    conduct_far,
    out_solution,
    out_defect,
    rhs, rhs1, rhs2, scrap,
    cond, cond2, gain0, gain1, gain2,
    a1, a2, a3, a4, a5, fd,
    m1, m2, m3, m4,
    k1, k2, k3, k4,
    halo_z, halo_x, halo_z2, halo_x2,
    source, conduct,
    in_send, in_recv, own_sem, load_sem,
    h_send, h_recv,
    out_send, out_recv, out_own,
):
    planes, rows, lanes = source.shape
    block = rows // peers
    half_planes, half_block = planes // 2, block // 2
    me, slab = lax.axis_index("tm"), lax.axis_index("space")
    mine = snake(me)
    following, preceding = snake((mine + 1) % peers), snake((mine + peers - 1) % peers)
    has_next, has_prev = mine < peers - 1, mine > 0
    has_up, has_down = slab < slabs - 1, slab > 0

    load_source = pltpu.make_async_copy(source_far, source, load_sem.at[0])
    load_conduct = pltpu.make_async_copy(conduct_far, conduct, load_sem.at[1])
    load_source.start()
    load_conduct.start()
    barrier = pltpu.get_barrier_semaphore()
    for k in range(1, peers):
        pl.semaphore_signal(
            barrier, inc=1, device_id={"tm": me ^ k}, device_id_type=MESH
        )

    @pl.when(has_up)
    def _():
        pl.semaphore_signal(barrier, inc=1, device_id={"space": slab + 1}, device_id_type=MESH)

    @pl.when(has_down)
    def _():
        pl.semaphore_signal(barrier, inc=1, device_id={"space": slab - 1}, device_id_type=MESH)

    neighbours = jnp.where(has_up, 1, 0) + jnp.where(has_down, 1, 0)
    load_source.wait()
    pl.semaphore_wait(barrier, peers - 1 + neighbours)

    def rows_of(index):
        return pl.ds(pl.multiple_of(snake(index) * block, 8), block)

    def inward(peer, step, recv):
        return pltpu.make_async_remote_copy(
            src_ref=source.at[:, rows_of(peer), :],
            dst_ref=rhs.at[:, :, step, :],
            send_sem=in_send.at[peer],
            recv_sem=in_recv.at[recv],
            device_id={"tm": peer},
            device_id_type=MESH,
        )

    order = sorted(range(1, peers), reverse=True)
    for k in order:
        inward(me ^ k, me, me).start()
    own = pltpu.make_async_copy(
        source_far.at[:, rows_of(me), :], rhs.at[:, :, me, :], own_sem
    )
    own.start()

    load_conduct.wait()

    def fill(z, _):
        for x in range(block):
            row = conduct[z, pl.ds(mine * block + x, 1), :]
            value = jnp.broadcast_to(row, (peers, lanes))
            cond[z, x] = value
            gain0[z, x] = OMEGA / (1.0 + value * (2.0 * sum(FINE)))
            gain1[z, x] = OMEGA / (1.0 + value * (4.0 * sum(FINE)))
        return 0

    lax.fori_loop(0, planes, fill, 0)

    def fill2(z, _):
        for x in range(half_block):
            value = 0.25 * (
                (cond[2 * z, 2 * x] + cond[2 * z + 1, 2 * x])
                + (cond[2 * z, 2 * x + 1] + cond[2 * z + 1, 2 * x + 1])
            )
            cond2[z, x] = value
            gain2[z, x] = OMEGA / (1.0 + value * (8.0 * sum(COARSE)))
        return 0

    lax.fori_loop(0, half_planes, fill2, 0)
    for ref in (a1, a2, a3, a4, a5, m1, m2, m3, m4, k1, k2, k3):
        depth, width = ref.shape[0], ref.shape[1]
        face = jnp.zeros((width, peers, lanes), jnp.float32)
        ref[0] = face
        ref[depth - 1] = face
        cell = jnp.zeros((peers, lanes), jnp.float32)

        def edge(z, _):
            ref[z, 0] = cell
            ref[z, width - 1] = cell
            return 0

        lax.fori_loop(1, depth - 1, edge, 0)

    time = lax.broadcasted_iota(jnp.int32, (1, peers, lanes), 1)
    lane = lax.broadcasted_iota(jnp.int32, (1, peers, lanes), 2)
    not_first, not_last = lane > 0, lane < lanes - 1

    def prior(value, shift):
        return jnp.where(time >= shift, pltpu.roll(value, shift, 1), 0.0)

    def with_partner(value, shift):
        even = (time // shift) % 2 == 0
        return value + jnp.where(
            even, pltpu.roll(value, peers - shift, 1), pltpu.roll(value, shift, 1)
        )

    def residual(ref, z, right, conductivity, weights, shift):
        weight_z, weight_x, weight_y = weights
        width = ref.shape[1] - 2
        inner = slice(1, width + 1)
        centre = ref[z + 1, inner]
        along_z = ref[z, inner] + ref[z + 2, inner]
        along_x = ref[z + 1, 0:width] + ref[z + 1, 2 : width + 2]
        along_y = jnp.where(not_first, pltpu.roll(centre, 1, 2), 0.0) + jnp.where(
            not_last, pltpu.roll(centre, lanes - 1, 2), 0.0
        )
        if weight_z == weight_x == weight_y:
            around = weight_z * (6.0 * centre - (along_z + along_x + along_y))
        else:
            around = (2.0 * (weight_z + weight_x + weight_y)) * centre - (
                weight_z * along_z + weight_x * along_x + weight_y * along_y
            )
        return centre, right + prior(centre, shift) - centre - conductivity * around

    def sweep(new, old, right, conductivity, gain, weights, shift):
        width = old.shape[1] - 2

        def plane(z, _):
            centre, left = residual(old, z, right[z], conductivity[z], weights, shift)
            new[z + 1, 1 : width + 1] = centre + gain[z] * left
            return 0

        lax.fori_loop(0, old.shape[0] - 2, plane, 0)

    def defect_into(new, off, old, right, conductivity, weights, shift):
        width = old.shape[1] - 2

        def plane(z, _):
            new[z + off, off : width + off] = residual(
                old, z, right[z], conductivity[z], weights, shift
            )[1]
            return 0

        lax.fori_loop(0, old.shape[0] - 2, plane, 0)

    def bufs(ref):
        if ref.shape[0] == planes + 2:
            return halo_z, halo_x
        return halo_z2, halo_x2

    def faces(ref, stage):
        into_z, into_x = bufs(ref)
        slot = stage_slot[stage]
        depth, width = ref.shape[0] - 2, ref.shape[1] - 2
        inner, deep = pl.ds(1, width), pl.ds(1, depth)

        def copy(src, dst, side, device):
            return pltpu.make_async_remote_copy(
                src_ref=src,
                dst_ref=dst,
                send_sem=h_send.at[stage, side],
                recv_sem=h_recv.at[stage, side],
                device_id=device,
                device_id_type=MESH,
            )

        return (
            (has_up, has_down, copy(ref.at[depth, inner], into_z.at[slot, 0], 0, {"space": slab + 1})),
            (has_down, has_up, copy(ref.at[1, inner], into_z.at[slot, 1], 1, {"space": slab - 1})),
            (has_next, has_prev, copy(ref.at[deep, width], into_x.at[slot, 0], 2, {"tm": following})),
            (has_prev, has_next, copy(ref.at[deep, 1], into_x.at[slot, 1], 3, {"tm": preceding})),
        )

    stage_slot = {0: 0, 1: 1, 2: 2, 3: 3, 4: 0, 5: 1, 6: 2, 7: 4, 8: 5, 9: 6, 10: 7, 11: 8}
    sent = []

    def send(ref, stage):
        for sends, _, copy in faces(ref, stage):
            pl.when(sends)(copy.start)
        sent.append((ref, stage))

    def receive(ref, stage, new, off, conductivity, gain, weights):
        weight_z, weight_x, _ = weights
        into_z, into_x = bufs(ref)
        slot = stage_slot[stage]
        depth, width = ref.shape[0] - 2, ref.shape[1] - 2
        inner, deep = slice(off, off + width), slice(off, off + depth)
        four = faces(ref, stage)

        def scale(*index):
            value = conductivity[index]
            return value if gain is None else value * gain[index]

        for side, z in ((0, 0), (1, depth - 1)):
            _, arrives, copy = four[side]

            @pl.when(arrives)
            def _(copy=copy, side=side, z=z):
                copy.wait_recv()
                new[z + off, inner] += scale(z) * (weight_z * into_z[slot, side])

        for side, x in ((0, 0), (1, width - 1)):
            _, arrives, copy = four[side + 2]

            @pl.when(arrives)
            def _(copy=copy, side=side, x=x):
                copy.wait_recv()
                new[deep, x + off] += scale(slice(None), x) * (weight_x * into_x[slot, side])

    fine, middle, coarse = FINE, scaled(FINE, 2.0), scaled(COARSE, 4.0)

    def edges_first(depth, width, work, between):
        work(0, 0, width)
        work(depth - 1, 0, width)

        def sides(z, _):
            work(z, 0, 1)
            work(z, width - 1, 1)
            return 0

        lax.fori_loop(1, depth - 1, sides, 0)
        between()

        def rest(z, _):
            work(z, 1, width - 2)
            return 0

        lax.fori_loop(1, depth - 1, rest, 0)

    own.wait()
    for k in order:
        inward(me, me ^ k, me ^ k).wait_recv()

    def first(z, x, count):
        at = slice(x, x + count)
        a1[z + 1, x + 1 : x + 1 + count] = gain0[z, at] * rhs[z, at]

    edges_first(planes, block, first, lambda: send(a1, 0))
    sweep(a2, a1, rhs, cond, gain0, fine, 1)
    receive(a1, 0, a2, 1, cond, gain0, fine)
    send(a2, 1)
    defect_into(scrap, 0, a2, rhs, cond, fine, 1)
    receive(a2, 1, scrap, 0, cond, None, fine)

    def restrict_time(z, x, count):
        at = slice(x, x + count)
        value = with_partner(scrap[z, at], 1)
        rhs1[z, at] = value
        m1[z + 1, x + 1 : x + 1 + count] = gain1[z, at] * value

    edges_first(planes, block, restrict_time, lambda: send(m1, 2))
    sweep(m2, m1, rhs1, cond, gain1, middle, 2)
    receive(m1, 2, m2, 1, cond, gain1, middle)
    send(m2, 3)
    defect_into(scrap, 0, m2, rhs1, cond, middle, 2)
    receive(m2, 3, scrap, 0, cond, None, middle)

    def restrict(z, _):
        for x in range(half_block):
            quad = (scrap[2 * z, 2 * x] + scrap[2 * z + 1, 2 * x]) + (
                scrap[2 * z, 2 * x + 1] + scrap[2 * z + 1, 2 * x + 1]
            )
            value = 0.25 * with_partner(quad[None], 2)[0]
            rhs2[z, x] = value
            k1[z + 1, x + 1] = gain2[z, x] * value
        return 0

    lax.fori_loop(0, half_planes, restrict, 0)
    send(k1, 4)
    sweep(k2, k1, rhs2, cond2, gain2, coarse, 4)
    receive(k1, 4, k2, 1, cond2, gain2, coarse)
    send(k2, 5)
    sweep(k3, k2, rhs2, cond2, gain2, coarse, 4)
    receive(k2, 5, k3, 1, cond2, gain2, coarse)
    send(k3, 6)
    sweep(k4, k3, rhs2, cond2, gain2, coarse, 4)
    receive(k3, 6, k4, 1, cond2, gain2, coarse)

    def prolong(z, x, count):
        for near in range(x, x + count):
            value = k4[z + 1, near + 1]
            for dz in range(2):
                for dx in range(2):
                    at = (2 * z + dz + 1, 2 * near + dx + 1)
                    m3[at] = m2[at] + value

    edges_first(half_planes, half_block, prolong, lambda: send(m3, 7))
    sweep(m4, m3, rhs1, cond, gain1, middle, 2)
    receive(m3, 7, m4, 1, cond, gain1, middle)
    send(m4, 8)

    def last_middle(z, _):
        centre, left = residual(m4, z, rhs1[z], cond[z], middle, 2)
        inner = slice(1, block + 1)
        a3[z + 1, inner] = a2[z + 1, inner] + (centre + gain1[z] * left)
        return 0

    lax.fori_loop(0, planes, last_middle, 0)
    receive(m4, 8, a3, 1, cond, gain1, middle)
    send(a3, 9)
    sweep(a4, a3, rhs, cond, gain0, fine, 1)
    receive(a3, 9, a4, 1, cond, gain0, fine)
    whole = (0, planes, 0, block)
    centre_part = (1, planes - 2, 1, block - 2)
    edge_parts = (
        (0, 1, 0, block),
        (planes - 1, 1, 0, block),
        (1, planes - 2, 0, 1),
        (1, planes - 2, block - 1, 1),
    )
    pieces = [(a5, 1, out_solution, part) for part in (centre_part,) + edge_parts]
    pieces.append((fd, 0, out_defect, whole))

    def ends(piece, step, owner):
        src, off, dst, (z, deep, x, wide) = pieces[piece]
        return (
            src.at[pl.ds(z + off, deep), pl.ds(x + off, wide), step, :],
            dst.at[pl.ds(z, deep), pl.ds(snake(owner) * block + x, wide), :],
        )

    def outward(piece, peer, owner):
        src, dst = ends(piece, peer, owner)
        return pltpu.make_async_remote_copy(
            src_ref=src,
            dst_ref=dst,
            send_sem=out_send.at[piece, peer],
            recv_sem=out_recv.at[piece, owner],
            device_id={"tm": peer},
            device_id_type=MESH,
        )

    def home(piece):
        src, dst = ends(piece, me, me)
        return pltpu.make_async_copy(src, dst, out_own.at[piece])

    def ship(piece):
        for k in order:
            outward(piece, me ^ k, me).start()
        home(piece).start()

    send(a4, 10)
    sweep(a5, a4, rhs, cond, gain0, fine, 1)
    ship(0)
    receive(a4, 10, a5, 1, cond, gain0, fine)
    send(a5, 11)
    for piece in range(1, 5):
        ship(piece)
    defect_into(fd, 0, a5, rhs, cond, fine, 1)
    receive(a5, 11, fd, 0, cond, None, fine)
    ship(5)

    for ref, stage in sent:
        for sends, _, copy in faces(ref, stage):
            pl.when(sends)(copy.wait_send)
    for k in order:
        inward(me ^ k, me, me).wait_send()
    for piece in range(6):
        home(piece).wait()
        for k in order:
            outward(piece, me ^ k, me).wait_send()
            outward(piece, me, me ^ k).wait_recv()


def fused_body(peers, slabs, source, conductivity):
    _, planes, rows, lanes = source.shape
    block = rows // peers

    def field(depth, width):
        return pltpu.VMEM((depth, width, peers, lanes), jnp.float32)

    plain, framed = field(planes, block), field(planes + 2, block + 2)
    small, small_framed = (
        field(planes // 2, block // 2),
        field(planes // 2 + 2, block // 2 + 2),
    )
    dma = pltpu.SemaphoreType.DMA
    anywhere = pl.BlockSpec(memory_space=pl.ANY)
    slab = pltpu.VMEM((planes, rows, lanes), jnp.float32)
    shape = jax.ShapeDtypeStruct((planes, rows, lanes), jnp.float32)

    def faces_of(slots, depth):
        return pltpu.VMEM((slots, 2, depth, peers, lanes), jnp.float32)

    solution, final_defect = pl.pallas_call(
        functools.partial(cycle_kernel, peers, slabs),
        out_shape=(shape, shape),
        in_specs=[anywhere, anywhere],
        out_specs=(anywhere, anywhere),
        scratch_shapes=[
            plain, plain, small, plain,
            plain, small, plain, plain, small,
            framed, framed, framed, framed, framed, plain,
            framed, framed, framed, framed,
            small_framed, small_framed, small_framed, small_framed,
            faces_of(9, block), faces_of(9, planes),
            faces_of(3, block // 2), faces_of(3, planes // 2),
            slab, slab,
            dma((peers,)), dma((peers,)), dma, dma((2,)),
            dma((12, 4)), dma((12, 4)),
            dma((6, peers)), dma((6, peers)), dma((6,)),
        ],
        compiler_params=pltpu.CompilerParams(
            collective_id=0, has_side_effects=True, vmem_limit_bytes=60 * 1024 * 1024
        ),
    )(source[0], conductivity)
    return (solution[None], final_defect[None])


def solution(mesh):
    peers, slabs = mesh.shape["tm"], mesh.shape["space"]

    def chosen(source, conductivity):
        steps, planes, rows, lanes = source.shape
        if fits(steps * peers, peers, slabs, planes, rows, lanes):
            return fused_body(peers, slabs, source, conductivity)
        return body(source, conductivity)

    return jax.shard_map(
        chosen,
        mesh=mesh,
        in_specs=(P("tm", "space", None, None), P("space", None, None)),
        out_specs=(P("tm", "space", None, None), P("tm", "space", None, None)),
        check_vma=False,
    )
```

```python
import functools

import jax
import jax.numpy as jnp
from jax import lax
from jax.experimental import pallas as pl
from jax.experimental.pallas import tpu as pltpu
from jax.sharding import PartitionSpec as P

NU = 2
NC = 4


OMEGA = 0.8
FINE = (1.0, 1.0, 1.0)
COARSE = (0.25, 0.25, 1.0)


def padded_2(shard, sides, width):
    for axis, dim in sides:
        peers, length = (lax.axis_size(axis), shard.shape[dim])
        up = [(i, (i + 1) % peers) for i in range(peers - 1)]
        down = [(j, i) for i, j in up]
        last = lax.slice_in_dim(shard, length - width, length, axis=dim)
        first = lax.slice_in_dim(shard, 0, width, axis=dim)
        before = lax.ppermute(last, axis, up)
        after = lax.ppermute(first, axis, down)
        shard = jnp.concatenate([before, shard, after], axis=dim)
    return shard


def shifted(shard, axis, by):
    peers = lax.axis_size(axis)
    pairs = [(i, i + by) for i in range(peers) if 0 <= i + by < peers]
    return lax.ppermute(shard, axis, pairs)


def swapped(value, axis, bit):
    mask = 2**bit
    pairs = [(source, source ^ mask) for source in range(lax.axis_size(axis))]
    return lax.ppermute(value, axis, pairs)


def stencil(padded, weights):
    weight_z, weight_x, weight_y = weights
    centre = padded[1:-1, :, 1:-1]
    widened = jnp.pad(padded[1:-1], ((0, 0), (1, 1), (0, 0)))
    along_z = 2.0 * centre - padded[2:, :, 1:-1] - padded[:-2, :, 1:-1]
    along_x = 2.0 * centre - widened[:, 2:, 1:-1] - widened[:, :-2, 1:-1]
    along_y = 2.0 * centre - padded[1:-1, :, 2:] - padded[1:-1, :, :-2]
    return weight_z * along_z + weight_x * along_x + weight_y * along_y


def defect(current, right_side, earlier, padded, conduct, stretch, weights):
    applied = current + stretch * conduct * stencil(padded, weights)
    return right_side + earlier - applied


def relaxed(current, right_side, earlier, padded, conduct, stretch, weights):
    weight_sum = 2.0 * (weights[0] + weights[1] + weights[2])
    diagonal = 1.0 + stretch * conduct * weight_sum
    return (
        current
        + OMEGA * defect(current, right_side, earlier, padded, conduct, stretch, weights) / diagonal
    )


def coarsen(values):
    return 0.25 * (
        values[..., 0::2, 0::2, :]
        + values[..., 1::2, 0::2, :]
        + (values[..., 0::2, 1::2, :] + values[..., 1::2, 1::2, :])
    )


def refine(values):
    return jnp.repeat(jnp.repeat(values, 2, axis=-3), 2, axis=-2)


def zero_columns(values):
    return jnp.pad(values, ((0, 0), (0, 0), (1, 1)))


def plane_faces(values):
    return padded_2(values, (("space", 0),), 1)


def coarse_planes_framed(values):
    return padded_2(values, (("space", 0),), 1)


def fine_frame(values):
    return zero_columns(plane_faces(values))


def step_prior(values):
    return shifted(values, "tm", 1)


def pair_prior(values):
    return shifted(values, "tm", 2)


def group_prior(values):
    return shifted(values, "tm", 4)


def smooth(current, right_side, conduct, stretch, weights, repeats, earlier_of, framing):
    for turn_index in range(repeats):
        current = relaxed(
            current, right_side, earlier_of(current), framing(current), conduct, stretch, weights
        )
    return current


def body(source, conductivity):
    right_side = source[0]
    solution = smooth(
        jnp.zeros_like(right_side), right_side, conductivity, 1.0, FINE, NU, step_prior, fine_frame
    )
    defect_fine = defect(
        solution, right_side, step_prior(solution), fine_frame(solution), conductivity, 1.0, FINE
    )
    middle_full = defect_fine + swapped(defect_fine, "tm", 0)
    middle = smooth(
        jnp.zeros_like(middle_full),
        middle_full,
        conductivity,
        2.0,
        FINE,
        NU,
        pair_prior,
        fine_frame,
    )
    middle_defect = defect(
        middle, middle_full, pair_prior(middle), fine_frame(middle), conductivity, 2.0, FINE
    )
    summed = middle_defect + swapped(middle_defect, "tm", 1)
    coarse_rhs = coarsen(summed)
    coarse_cond = coarsen(conductivity)

    def coarse_frame(values):
        return zero_columns(coarse_planes_framed(values))

    coarse = smooth(
        jnp.zeros_like(coarse_rhs),
        coarse_rhs,
        coarse_cond,
        4.0,
        COARSE,
        NC,
        group_prior,
        coarse_frame,
    )
    middle = middle + refine(coarse)
    middle = smooth(middle, middle_full, conductivity, 2.0, FINE, NU, pair_prior, fine_frame)
    solution = solution + middle
    solution = smooth(solution, right_side, conductivity, 1.0, FINE, NU, step_prior, fine_frame)
    final_defect = defect(
        solution, right_side, step_prior(solution), fine_frame(solution), conductivity, 1.0, FINE
    )
    return (solution[None], final_defect[None])


MESH = pl.DeviceIdType.MESH


def snake(index):
    return index + ((index // 2) % 2) * (1 - 2 * (index % 2))


def scaled(weights, stretch):
    return tuple(stretch * weight for weight in weights)


def fits(steps, peers, slabs, planes, rows, lanes):
    block = rows // peers
    return (
        steps == peers
        and peers % 8 == 0
        and peers & (peers - 1) == 0
        and rows % peers == 0
        and block % 8 == 0
        and planes % 2 == 0
        and planes >= 6
        and lanes % 128 == 0
        and peers <= 16
        and slabs > 1
    )


PAD, PAD2 = 2, 3


def cycle_kernel(
    peers,
    slabs,
    source_far,
    conduct_far,
    out_solution,
    out_defect,
    rhs, rhs1, rhs2, scrap,
    cond, cond2, gain0, gain1, gain2,
    a1, a2, a3, a4, a5, fd,
    m1, m2, m3, m4,
    k1, k2, k3, k4,
    source, tall,
    in_send, in_recv, own_sem, load_sem,
    tall_send, tall_recv,
    h_send, h_recv,
    out_send, out_recv, out_own,
):
    planes, rows, lanes = source.shape
    block = rows // peers
    half_planes, half_block = planes // 2, block // 2
    reach = 2 * PAD2
    me, slab = lax.axis_index("tm"), lax.axis_index("space")
    mine = snake(me)
    following, preceding = snake((mine + 1) % peers), snake((mine + peers - 1) % peers)
    has_z = {1: slab < slabs - 1, -1: slab > 0, 0: None}
    has_x = {1: mine < peers - 1, -1: mine > 0, 0: None}
    beside = {1: following, -1: preceding}

    def both(first, second):
        if first is None:
            return second
        return first if second is None else first & second

    def device(dz, dx):
        where = {}
        if dx:
            where["tm"] = beside[dx]
        if dz:
            where["space"] = slab + dz
        return where

    def size_of(ref):
        pad = PAD2 if ref.shape[0] == half_planes + 2 * PAD2 else PAD
        return pad, ref.shape[0] - 2 * pad, ref.shape[1] - 2 * pad

    def box(ref, ring):
        pad, depth, width = size_of(ref)
        return (pad - ring, pad + depth + ring, pad - ring, pad + width + ring)

    def strips(ref, outer, inner):
        z0, z1, x0, x1 = box(ref, outer)
        i0, i1, j0, j1 = box(ref, inner)
        return ((z0, i0, x0, x1), (i1, z1, x0, x1), (i0, i1, x0, j0), (i0, i1, j1, x1))

    def over(boxes, work):
        for z0, z1, x0, x1 in boxes:

            def step(z, _, x0=x0, x1=x1):
                work(z, x0, x1)
                return 0

            lax.fori_loop(z0, z1, step, 0)

    load_source = pltpu.make_async_copy(source_far, source, load_sem.at[0])
    load_conduct = pltpu.make_async_copy(
        conduct_far, tall.at[pl.ds(reach, planes)], load_sem.at[1]
    )
    load_source.start()
    load_conduct.start()

    for ref in (rhs, rhs1, m3, a3, a5, rhs2):

        def clear(z, x0, x1, ref=ref):
            ref[z, x0:x1] = jnp.zeros((x1 - x0, peers, lanes), jnp.float32)

        over(strips(ref, size_of(ref)[0], 0), clear)

    barrier = pltpu.get_barrier_semaphore()
    for k in range(1, peers):
        pl.semaphore_signal(barrier, inc=1, device_id={"tm": me ^ k}, device_id_type=MESH)
    expected = peers - 1
    for dz in (1, -1):
        for dx in (0, 1, -1):
            here = both(has_z[dz], has_x[dx])

            @pl.when(here)
            def _(dz=dz, dx=dx):
                pl.semaphore_signal(
                    barrier, inc=1, device_id=device(dz, dx), device_id_type=MESH
                )

            expected = expected + jnp.where(here, 1, 0)
    load_source.wait()
    pl.semaphore_wait(barrier, expected)

    def rows_of(index):
        return pl.ds(pl.multiple_of(snake(index) * block, 8), block)

    def inward(peer, step, recv):
        return pltpu.make_async_remote_copy(
            src_ref=source.at[:, rows_of(peer), :],
            dst_ref=rhs.at[pl.ds(PAD, planes), pl.ds(PAD, block), step, :],
            send_sem=in_send.at[peer],
            recv_sem=in_recv.at[recv],
            device_id={"tm": peer},
            device_id_type=MESH,
        )

    order = sorted(range(1, peers), reverse=True)
    for k in order:
        inward(me ^ k, me, me).start()
    own = pltpu.make_async_copy(
        source_far.at[:, rows_of(me), :],
        rhs.at[pl.ds(PAD, planes), pl.ds(PAD, block), me, :],
        own_sem,
    )
    own.start()
    load_conduct.wait()

    def tall_copy(side, dz):
        src = planes if dz > 0 else reach
        dst = 0 if dz > 0 else reach + planes
        return pltpu.make_async_remote_copy(
            src_ref=tall.at[pl.ds(src, reach)],
            dst_ref=tall.at[pl.ds(dst, reach)],
            send_sem=tall_send.at[side],
            recv_sem=tall_recv.at[side],
            device_id={"space": slab + dz},
            device_id_type=MESH,
        )

    for side, dz in ((0, 1), (1, -1)):
        pl.when(has_z[dz])(tall_copy(side, dz).start)
    for side, dz in ((0, 1), (1, -1)):
        pl.when(has_z[-dz])(tall_copy(side, dz).wait_recv)

        @pl.when(jnp.logical_not(has_z[-dz]))
        def _(dz=dz):
            start = 0 if dz > 0 else reach + planes
            tall[start : start + reach] = jnp.zeros((reach, rows, lanes), jnp.float32)

    def inside(z, x, factor):
        plane = slab * (planes // factor) + z
        row = mine * (block // factor) + x
        ok = (plane >= 0) & (plane < slabs * planes // factor)
        ok = ok & (row >= 0) & (row < rows // factor)
        return jnp.where(ok, 1.0, 0.0)

    def fill(z, _):
        for x in range(block + 2 * PAD):
            row = jnp.clip(mine * block + x - PAD, 0, rows - 1)
            value = jnp.broadcast_to(tall[z + reach - PAD, pl.ds(row, 1), :], (peers, lanes))
            mask = inside(z - PAD, x - PAD, 1)
            cond[z, x] = value * mask
            gain0[z, x] = mask * (OMEGA / (1.0 + value * (2.0 * sum(FINE))))
            gain1[z, x] = mask * (OMEGA / (1.0 + value * (4.0 * sum(FINE))))
        return 0

    lax.fori_loop(0, planes + 2 * PAD, fill, 0)

    def fill2(z, _):
        for x in range(half_block + 2 * PAD2):
            row = jnp.clip(mine * block + 2 * (x - PAD2), 0, rows - 2)
            quad = (tall[2 * z, pl.ds(row, 1), :] + tall[2 * z + 1, pl.ds(row, 1), :]) + (
                tall[2 * z, pl.ds(row + 1, 1), :] + tall[2 * z + 1, pl.ds(row + 1, 1), :]
            )
            value = jnp.broadcast_to(0.25 * quad, (peers, lanes))
            mask = inside(z - PAD2, x - PAD2, 2)
            cond2[z, x] = value * mask
            gain2[z, x] = mask * (OMEGA / (1.0 + value * (8.0 * sum(COARSE))))
        return 0

    lax.fori_loop(0, half_planes + 2 * PAD2, fill2, 0)

    time = lax.broadcasted_iota(jnp.int32, (1, peers, lanes), 1)
    lane = lax.broadcasted_iota(jnp.int32, (1, peers, lanes), 2)
    not_first, not_last = lane > 0, lane < lanes - 1

    def prior(value, shift):
        return jnp.where(time >= shift, pltpu.roll(value, shift, 1), 0.0)

    def with_partner(value, shift):
        even = (time // shift) % 2 == 0
        return value + jnp.where(
            even, pltpu.roll(value, peers - shift, 1), pltpu.roll(value, shift, 1)
        )

    def residual(ref, z, x0, x1, right, conductivity, weights, shift):
        weight_z, weight_x, weight_y = weights
        at = slice(x0, x1)
        centre = ref[z, at]
        along_z = ref[z - 1, at] + ref[z + 1, at]
        along_x = ref[z, x0 - 1 : x1 - 1] + ref[z, x0 + 1 : x1 + 1]
        along_y = jnp.where(not_first, pltpu.roll(centre, 1, 2), 0.0) + jnp.where(
            not_last, pltpu.roll(centre, lanes - 1, 2), 0.0
        )
        if weight_z == weight_x == weight_y:
            around = weight_z * (6.0 * centre - (along_z + along_x + along_y))
        else:
            around = (2.0 * (weight_z + weight_x + weight_y)) * centre - (
                weight_z * along_z + weight_x * along_x + weight_y * along_y
            )
        left = right[z, at] + prior(centre, shift) - centre - conductivity[z, at] * around
        return centre, left

    def sweeper(new, old, right, conductivity, gain, weights, shift, base=None):
        def work(z, x0, x1):
            centre, left = residual(old, z, x0, x1, right, conductivity, weights, shift)
            value = centre + gain[z, x0:x1] * left
            new[z, x0:x1] = value if base is None else base[z, x0:x1] + value

        return work

    def starter(new, right, gain):
        def work(z, x0, x1):
            new[z, x0:x1] = gain[z, x0:x1] * right[z, x0:x1]

        return work

    def defecter(new, old, right, weights, shift, pairs):
        def work(z, x0, x1):
            left = residual(old, z, x0, x1, right, cond, weights, shift)[1]
            new[z, x0:x1] = with_partner(left, 1) if pairs else left

        return work

    def wide(ref, depth, corner, stage):
        pad, deep, broad = size_of(ref)

        def spans(step, size, count):
            if step == 0:
                return pl.ds(pad, size), pl.ds(pad, size)
            if step > 0:
                return pl.ds(pad + size - count, count), pl.ds(pad - count, count)
            return pl.ds(pad, count), pl.ds(pad + size, count)

        out = []
        steps = [(dz, dx) for dz in (1, -1) for dx in (1, -1)] if corner else []
        for number, (dz, dx) in enumerate(steps + [(0, 1), (0, -1), (1, 0), (-1, 0)]):
            count = corner if dz and dx else depth
            src_z, dst_z = spans(dz, deep, count)
            src_x, dst_x = spans(dx, broad, count)
            copy = pltpu.make_async_remote_copy(
                src_ref=ref.at[src_z, src_x],
                dst_ref=ref.at[dst_z, dst_x],
                send_sem=h_send.at[stage, number],
                recv_sem=h_recv.at[stage, number],
                device_id=device(dz, dx),
                device_id_type=MESH,
            )
            sends = both(has_z[dz], has_x[dx])
            arrives = both(has_z[-dz], has_x[-dx])
            out.append((sends, arrives, copy))
        return out

    started = []

    def send(ref, depth, corner, stage):
        copies = wide(ref, depth, corner, stage)
        for sends, _, copy in copies:
            pl.when(sends)(copy.start)
        started.append(copies)

    def receive():
        for _, arrives, copy in started[-1]:
            pl.when(arrives)(copy.wait_recv)

    fine, middle, coarse = FINE, scaled(FINE, 2.0), scaled(COARSE, 4.0)

    def pieces_of(ref, edge):
        _, deep, broad = size_of(ref)
        return (
            (edge, deep - 2 * edge, edge, broad - 2 * edge),
            (0, edge, 0, broad),
            (deep - edge, edge, 0, broad),
            (edge, deep - 2 * edge, 0, edge),
            (edge, deep - 2 * edge, broad - edge, edge),
        )

    pieces = [(a5, out_solution, part) for part in pieces_of(a5, 2)]
    pieces.append((fd, out_defect, (0, planes, 0, block)))

    def ends(piece, step, owner):
        src, dst, (z, deep, x, broad) = pieces[piece]
        return (
            src.at[pl.ds(z + PAD, deep), pl.ds(x + PAD, broad), step, :],
            dst.at[pl.ds(z, deep), pl.ds(snake(owner) * block + x, broad), :],
        )

    def outward(piece, peer, owner):
        src, dst = ends(piece, peer, owner)
        return pltpu.make_async_remote_copy(
            src_ref=src,
            dst_ref=dst,
            send_sem=out_send.at[piece, peer],
            recv_sem=out_recv.at[piece, owner],
            device_id={"tm": peer},
            device_id_type=MESH,
        )

    def home(piece):
        src, dst = ends(piece, me, me)
        return pltpu.make_async_copy(src, dst, out_own.at[piece])

    def ship(piece):
        for k in order:
            outward(piece, me ^ k, me).start()
        home(piece).start()

    def stages(boxes_of, works):
        for work, (ref, rings) in zip(works, boxes_of):
            over(strips(ref, *rings) if isinstance(rings, tuple) else (box(ref, rings),), work)

    def presmooth(x, right, one, two, left, gain, weights, shift, pairs):
        works = (
            starter(one, right, gain),
            sweeper(two, one, right, cond, gain, weights, shift),
            defecter(left, two, right, weights, shift, pairs),
        )
        send(right, 2, 1, x)
        stages(((one, 0), (two, -1), (left, -2)), works)
        receive()
        stages(((one, (2, 0)), (two, (1, -1)), (left, (0, -2))), works)

    own.wait()
    for k in order:
        inward(me, me ^ k, me ^ k).wait_recv()
    presmooth(0, rhs, a1, a2, rhs1, gain0, fine, 1, True)
    presmooth(1, rhs1, m1, m2, scrap, gain1, middle, 2, False)

    def restrict(z, _):
        for x in range(half_block):
            zz, xx = 2 * z + PAD, 2 * x + PAD
            quad = (scrap[zz, xx] + scrap[zz + 1, xx]) + (
                scrap[zz, xx + 1] + scrap[zz + 1, xx + 1]
            )
            rhs2[z + PAD2, x + PAD2] = 0.25 * with_partner(quad[None], 2)[0]
        return 0

    lax.fori_loop(0, half_planes, restrict, 0)
    send(rhs2, 3, 2, 2)
    start = starter(k1, rhs2, gain2)
    works = [
        sweeper(new, old, rhs2, cond2, gain2, coarse, 4)
        for new, old in ((k2, k1), (k3, k2), (k4, k3))
    ]
    stages(((k1, 0), (k2, -1)), (start, works[0]))
    receive()
    stages(((k1, (3, 0)), (k2, (2, -1)), (k3, 1), (k4, 0)), (start, *works))

    def prolong(z, x0, x1):
        for x in range(x0, x1):
            value = k4[z, x]
            for dz in range(2):
                for dx in range(2):
                    at = (2 * (z - PAD2) + dz + PAD, 2 * (x - PAD2) + dx + PAD)
                    m3[at] = m2[at] + value

    over(strips(k4, 0, -1), prolong)
    send(m3, 2, 1, 3)
    over((box(k4, -1),), prolong)
    works = (
        sweeper(m4, m3, rhs1, cond, gain1, middle, 2),
        sweeper(a3, m4, rhs1, cond, gain1, middle, 2, a2),
    )
    stages(((m4, -1), (a3, -2)), works)
    receive()
    stages(((m4, (1, -1)), (a3, (0, -2))), works)
    send(a3, 2, 1, 4)
    works = (
        sweeper(a4, a3, rhs, cond, gain0, fine, 1),
        sweeper(a5, a4, rhs, cond, gain0, fine, 1),
    )
    stages(((a4, -1), (a5, -2)), works)
    ship(0)
    receive()
    stages(((a4, (1, -1)), (a5, (0, -2))), works)
    send(a5, 1, 0, 5)
    for piece in range(1, 5):
        ship(piece)
    works = (defecter(fd, a5, rhs, fine, 1, False),)
    stages(((fd, -1),), works)
    receive()
    stages(((fd, (0, -1)),), works)
    ship(5)

    for copies in started:
        for sends, _, copy in copies:
            pl.when(sends)(copy.wait_send)
    for side, dz in ((0, 1), (1, -1)):
        pl.when(has_z[dz])(tall_copy(side, dz).wait_send)
    for k in order:
        inward(me ^ k, me, me).wait_send()
    for piece in range(6):
        home(piece).wait()
        for k in order:
            outward(piece, me ^ k, me).wait_send()
            outward(piece, me, me ^ k).wait_recv()


def fused_body(peers, slabs, source, conductivity):
    _, planes, rows, lanes = source.shape
    block = rows // peers

    def field(depth, width):
        return pltpu.VMEM((depth, width, peers, lanes), jnp.float32)

    large = field(planes + 2 * PAD, block + 2 * PAD)
    small = field(planes // 2 + 2 * PAD2, block // 2 + 2 * PAD2)
    dma = pltpu.SemaphoreType.DMA
    anywhere = pl.BlockSpec(memory_space=pl.ANY)
    shape = jax.ShapeDtypeStruct((planes, rows, lanes), jnp.float32)
    solution, final_defect = pl.pallas_call(
        functools.partial(cycle_kernel, peers, slabs),
        out_shape=(shape, shape),
        in_specs=[anywhere, anywhere],
        out_specs=(anywhere, anywhere),
        scratch_shapes=[
            large, large, small, large,
            large, small, large, large, small,
            large, large, large, large, large, large,
            large, large, large, large,
            small, small, small, small,
            pltpu.VMEM((planes, rows, lanes), jnp.float32),
            pltpu.VMEM((planes + 4 * PAD2, rows, lanes), jnp.float32),
            dma((peers,)), dma((peers,)), dma, dma((2,)),
            dma((2,)), dma((2,)),
            dma((6, 8)), dma((6, 8)),
            dma((6, peers)), dma((6, peers)), dma((6,)),
        ],
        compiler_params=pltpu.CompilerParams(
            collective_id=0, has_side_effects=True, vmem_limit_bytes=60 * 1024 * 1024
        ),
    )(source[0], conductivity)
    return (solution[None], final_defect[None])


def solution(mesh):
    peers, slabs = mesh.shape["tm"], mesh.shape["space"]

    def chosen(source, conductivity):
        steps, planes, rows, lanes = source.shape
        if fits(steps * peers, peers, slabs, planes, rows, lanes):
            return fused_body(peers, slabs, source, conductivity)
        return body(source, conductivity)

    return jax.shard_map(
        chosen,
        mesh=mesh,
        in_specs=(P("tm", "space", None, None), P("space", None, None)),
        out_specs=(P("tm", "space", None, None), P("tm", "space", None, None)),
        check_vma=False,
    )
```

```python
import functools

import jax
import jax.numpy as jnp
from jax import lax
from jax.experimental import pallas as pl
from jax.experimental.pallas import tpu as pltpu
from jax.sharding import PartitionSpec as P

NU = 2
NC = 4


OMEGA = 0.8
FINE = (1.0, 1.0, 1.0)
COARSE = (0.25, 0.25, 1.0)


def padded_2(shard, sides, width):
    for axis, dim in sides:
        peers, length = (lax.axis_size(axis), shard.shape[dim])
        up = [(i, (i + 1) % peers) for i in range(peers - 1)]
        down = [(j, i) for i, j in up]
        last = lax.slice_in_dim(shard, length - width, length, axis=dim)
        first = lax.slice_in_dim(shard, 0, width, axis=dim)
        before = lax.ppermute(last, axis, up)
        after = lax.ppermute(first, axis, down)
        shard = jnp.concatenate([before, shard, after], axis=dim)
    return shard


def shifted(shard, axis, by):
    peers = lax.axis_size(axis)
    pairs = [(i, i + by) for i in range(peers) if 0 <= i + by < peers]
    return lax.ppermute(shard, axis, pairs)


def swapped(value, axis, bit):
    mask = 2**bit
    pairs = [(source, source ^ mask) for source in range(lax.axis_size(axis))]
    return lax.ppermute(value, axis, pairs)


def stencil(padded, weights):
    weight_z, weight_x, weight_y = weights
    centre = padded[1:-1, :, 1:-1]
    widened = jnp.pad(padded[1:-1], ((0, 0), (1, 1), (0, 0)))
    along_z = 2.0 * centre - padded[2:, :, 1:-1] - padded[:-2, :, 1:-1]
    along_x = 2.0 * centre - widened[:, 2:, 1:-1] - widened[:, :-2, 1:-1]
    along_y = 2.0 * centre - padded[1:-1, :, 2:] - padded[1:-1, :, :-2]
    return weight_z * along_z + weight_x * along_x + weight_y * along_y


def defect(current, right_side, earlier, padded, conduct, stretch, weights):
    applied = current + stretch * conduct * stencil(padded, weights)
    return right_side + earlier - applied


def relaxed(current, right_side, earlier, padded, conduct, stretch, weights):
    weight_sum = 2.0 * (weights[0] + weights[1] + weights[2])
    diagonal = 1.0 + stretch * conduct * weight_sum
    return (
        current
        + OMEGA * defect(current, right_side, earlier, padded, conduct, stretch, weights) / diagonal
    )


def coarsen(values):
    return 0.25 * (
        values[..., 0::2, 0::2, :]
        + values[..., 1::2, 0::2, :]
        + (values[..., 0::2, 1::2, :] + values[..., 1::2, 1::2, :])
    )


def refine(values):
    return jnp.repeat(jnp.repeat(values, 2, axis=-3), 2, axis=-2)


def zero_columns(values):
    return jnp.pad(values, ((0, 0), (0, 0), (1, 1)))


def plane_faces(values):
    return padded_2(values, (("space", 0),), 1)


def coarse_planes_framed(values):
    return padded_2(values, (("space", 0),), 1)


def fine_frame(values):
    return zero_columns(plane_faces(values))


def step_prior(values):
    return shifted(values, "tm", 1)


def pair_prior(values):
    return shifted(values, "tm", 2)


def group_prior(values):
    return shifted(values, "tm", 4)


def smooth(current, right_side, conduct, stretch, weights, repeats, earlier_of, framing):
    for turn_index in range(repeats):
        current = relaxed(
            current, right_side, earlier_of(current), framing(current), conduct, stretch, weights
        )
    return current


def body(source, conductivity):
    right_side = source[0]
    solution = smooth(
        jnp.zeros_like(right_side), right_side, conductivity, 1.0, FINE, NU, step_prior, fine_frame
    )
    defect_fine = defect(
        solution, right_side, step_prior(solution), fine_frame(solution), conductivity, 1.0, FINE
    )
    middle_full = defect_fine + swapped(defect_fine, "tm", 0)
    middle = smooth(
        jnp.zeros_like(middle_full),
        middle_full,
        conductivity,
        2.0,
        FINE,
        NU,
        pair_prior,
        fine_frame,
    )
    middle_defect = defect(
        middle, middle_full, pair_prior(middle), fine_frame(middle), conductivity, 2.0, FINE
    )
    summed = middle_defect + swapped(middle_defect, "tm", 1)
    coarse_rhs = coarsen(summed)
    coarse_cond = coarsen(conductivity)

    def coarse_frame(values):
        return zero_columns(coarse_planes_framed(values))

    coarse = smooth(
        jnp.zeros_like(coarse_rhs),
        coarse_rhs,
        coarse_cond,
        4.0,
        COARSE,
        NC,
        group_prior,
        coarse_frame,
    )
    middle = middle + refine(coarse)
    middle = smooth(middle, middle_full, conductivity, 2.0, FINE, NU, pair_prior, fine_frame)
    solution = solution + middle
    solution = smooth(solution, right_side, conductivity, 1.0, FINE, NU, step_prior, fine_frame)
    final_defect = defect(
        solution, right_side, step_prior(solution), fine_frame(solution), conductivity, 1.0, FINE
    )
    return (solution[None], final_defect[None])


MESH = pl.DeviceIdType.MESH


def snake(index):
    return index + ((index // 2) % 2) * (1 - 2 * (index % 2))


def scaled(weights, stretch):
    return tuple(stretch * weight for weight in weights)


def fits(steps, peers, slabs, planes, rows, lanes):
    block = rows // peers
    return (
        steps == peers
        and peers % 8 == 0
        and peers & (peers - 1) == 0
        and rows % peers == 0
        and block % 8 == 0
        and planes % 2 == 0
        and planes >= 6
        and lanes % 128 == 0
        and peers <= 16
        and slabs > 1
    )


PAD, PAD2 = 2, 3


def cycle_kernel(
    peers,
    slabs,
    source_far,
    conduct_far,
    out_solution,
    out_defect,
    rhs, rhs1, rhs2, scrap,
    cond, cond2, gain0, gain1, gain2,
    a1, a2, a3, a4, a5, fd,
    m1, m2, m3, m4,
    k1, k2, k3, k4,
    source, tall,
    in_send, in_recv, own_sem, load_sem,
    tall_send, tall_recv,
    h_send, h_recv,
    out_send, out_recv, out_own,
):
    planes, rows, lanes = source.shape
    block = rows // peers
    half_planes, half_block = planes // 2, block // 2
    reach = 2 * PAD2
    me, slab = lax.axis_index("tm"), lax.axis_index("space")
    mine = snake(me)
    following, preceding = snake((mine + 1) % peers), snake((mine + peers - 1) % peers)
    has_z = {1: slab < slabs - 1, -1: slab > 0, 0: None}
    has_x = {1: mine < peers - 1, -1: mine > 0, 0: None}
    beside = {1: following, -1: preceding}

    def both(first, second):
        if first is None:
            return second
        return first if second is None else first & second

    def device(dz, dx):
        where = {}
        if dx:
            where["tm"] = beside[dx]
        if dz:
            where["space"] = slab + dz
        return where

    def size_of(ref):
        pad = PAD2 if ref.shape[0] == half_planes + 2 * PAD2 else PAD
        return pad, ref.shape[0] - 2 * pad, ref.shape[1] - 2 * pad

    def box(ref, ring):
        pad, depth, width = size_of(ref)
        return (pad - ring, pad + depth + ring, pad - ring, pad + width + ring)

    def strips(ref, outer, inner):
        z0, z1, x0, x1 = box(ref, outer)
        i0, i1, j0, j1 = box(ref, inner)
        return ((z0, i0, x0, x1), (i1, z1, x0, x1), (i0, i1, x0, j0), (i0, i1, j1, x1))

    def over(boxes, work):
        for z0, z1, x0, x1 in boxes:
            if z1 - z0 <= 2 or x1 - x0 <= 4:
                for z in range(z0, z1):
                    work(z, x0, x1)
                continue

            def step(z, _, x0=x0, x1=x1):
                work(z, x0, x1)
                return 0

            lax.fori_loop(z0, z1, step, 0)

    load_source = pltpu.make_async_copy(source_far, source, load_sem.at[0])
    load_conduct = pltpu.make_async_copy(
        conduct_far, tall.at[pl.ds(reach, planes)], load_sem.at[1]
    )
    load_source.start()
    load_conduct.start()

    for ref in (rhs, rhs1, m3, a3, a5, rhs2):

        def clear(z, x0, x1, ref=ref):
            ref[z, x0:x1] = jnp.zeros((x1 - x0, peers, lanes), jnp.float32)

        over(strips(ref, size_of(ref)[0], 0), clear)

    barrier = pltpu.get_barrier_semaphore()
    for k in range(1, peers):
        pl.semaphore_signal(barrier, inc=1, device_id={"tm": me ^ k}, device_id_type=MESH)
    expected = peers - 1
    for dz in (1, -1):
        for dx in (0, 1, -1):
            here = both(has_z[dz], has_x[dx])

            @pl.when(here)
            def _(dz=dz, dx=dx):
                pl.semaphore_signal(
                    barrier, inc=1, device_id=device(dz, dx), device_id_type=MESH
                )

            expected = expected + jnp.where(here, 1, 0)
    load_source.wait()
    pl.semaphore_wait(barrier, expected)

    def rows_of(index):
        return pl.ds(pl.multiple_of(snake(index) * block, 8), block)

    def inward(peer, step, recv):
        return pltpu.make_async_remote_copy(
            src_ref=source.at[:, rows_of(peer), :],
            dst_ref=rhs.at[pl.ds(PAD, planes), pl.ds(PAD, block), step, :],
            send_sem=in_send.at[peer],
            recv_sem=in_recv.at[recv],
            device_id={"tm": peer},
            device_id_type=MESH,
        )

    order = sorted(range(1, peers), reverse=True)
    for k in order:
        inward(me ^ k, me, me).start()
    own = pltpu.make_async_copy(
        source_far.at[:, rows_of(me), :],
        rhs.at[pl.ds(PAD, planes), pl.ds(PAD, block), me, :],
        own_sem,
    )
    own.start()
    load_conduct.wait()

    def tall_copy(side, dz):
        src = planes if dz > 0 else reach
        dst = 0 if dz > 0 else reach + planes
        return pltpu.make_async_remote_copy(
            src_ref=tall.at[pl.ds(src, reach)],
            dst_ref=tall.at[pl.ds(dst, reach)],
            send_sem=tall_send.at[side],
            recv_sem=tall_recv.at[side],
            device_id={"space": slab + dz},
            device_id_type=MESH,
        )

    for side, dz in ((0, 1), (1, -1)):
        pl.when(has_z[dz])(tall_copy(side, dz).start)
    for side, dz in ((0, 1), (1, -1)):
        pl.when(has_z[-dz])(tall_copy(side, dz).wait_recv)

        @pl.when(jnp.logical_not(has_z[-dz]))
        def _(dz=dz):
            start = 0 if dz > 0 else reach + planes
            tall[start : start + reach] = jnp.zeros((reach, rows, lanes), jnp.float32)

    def inside(z, x, factor):
        plane = slab * (planes // factor) + z
        row = mine * (block // factor) + x
        ok = (plane >= 0) & (plane < slabs * planes // factor)
        ok = ok & (row >= 0) & (row < rows // factor)
        return jnp.where(ok, 1.0, 0.0)

    def fill(z, _):
        for x in range(block + 2 * PAD):
            row = jnp.clip(mine * block + x - PAD, 0, rows - 1)
            value = jnp.broadcast_to(tall[z + reach - PAD, pl.ds(row, 1), :], (peers, lanes))
            mask = inside(z - PAD, x - PAD, 1)
            cond[z, x] = value * mask
            gain0[z, x] = mask * (OMEGA / (1.0 + value * (2.0 * sum(FINE))))
            gain1[z, x] = mask * (OMEGA / (1.0 + value * (4.0 * sum(FINE))))
        return 0

    lax.fori_loop(0, planes + 2 * PAD, fill, 0)

    def fill2(z, _):
        for x in range(half_block + 2 * PAD2):
            row = jnp.clip(mine * block + 2 * (x - PAD2), 0, rows - 2)
            quad = (tall[2 * z, pl.ds(row, 1), :] + tall[2 * z + 1, pl.ds(row, 1), :]) + (
                tall[2 * z, pl.ds(row + 1, 1), :] + tall[2 * z + 1, pl.ds(row + 1, 1), :]
            )
            value = jnp.broadcast_to(0.25 * quad, (peers, lanes))
            mask = inside(z - PAD2, x - PAD2, 2)
            cond2[z, x] = value * mask
            gain2[z, x] = mask * (OMEGA / (1.0 + value * (8.0 * sum(COARSE))))
        return 0

    lax.fori_loop(0, half_planes + 2 * PAD2, fill2, 0)

    time = lax.broadcasted_iota(jnp.int32, (1, peers, lanes), 1)
    lane = lax.broadcasted_iota(jnp.int32, (1, peers, lanes), 2)
    not_first, not_last = lane > 0, lane < lanes - 1

    def prior(value, shift):
        return jnp.where(time >= shift, pltpu.roll(value, shift, 1), 0.0)

    def with_partner(value, shift):
        even = (time // shift) % 2 == 0
        return value + jnp.where(
            even, pltpu.roll(value, peers - shift, 1), pltpu.roll(value, shift, 1)
        )

    def residual(ref, z, x0, x1, right, conductivity, weights, shift):
        weight_z, weight_x, weight_y = weights
        at = slice(x0, x1)
        centre = ref[z, at]
        along_z = ref[z - 1, at] + ref[z + 1, at]
        along_x = ref[z, x0 - 1 : x1 - 1] + ref[z, x0 + 1 : x1 + 1]
        along_y = jnp.where(not_first, pltpu.roll(centre, 1, 2), 0.0) + jnp.where(
            not_last, pltpu.roll(centre, lanes - 1, 2), 0.0
        )
        if weight_z == weight_x == weight_y:
            around = weight_z * (6.0 * centre - (along_z + along_x + along_y))
        else:
            around = (2.0 * (weight_z + weight_x + weight_y)) * centre - (
                weight_z * along_z + weight_x * along_x + weight_y * along_y
            )
        left = right[z, at] + prior(centre, shift) - centre - conductivity[z, at] * around
        return centre, left

    def sweeper(new, old, right, conductivity, gain, weights, shift, base=None):
        def work(z, x0, x1):
            centre, left = residual(old, z, x0, x1, right, conductivity, weights, shift)
            value = centre + gain[z, x0:x1] * left
            new[z, x0:x1] = value if base is None else base[z, x0:x1] + value

        return work

    def starter(new, right, gain):
        def work(z, x0, x1):
            new[z, x0:x1] = gain[z, x0:x1] * right[z, x0:x1]

        return work

    def defecter(new, old, right, weights, shift, pairs):
        def work(z, x0, x1):
            left = residual(old, z, x0, x1, right, cond, weights, shift)[1]
            new[z, x0:x1] = with_partner(left, 1) if pairs else left

        return work

    def wide(ref, depth, corner, stage):
        pad, deep, broad = size_of(ref)

        def spans(step, size, count):
            if step == 0:
                return pl.ds(pad, size), pl.ds(pad, size)
            if step > 0:
                return pl.ds(pad + size - count, count), pl.ds(pad - count, count)
            return pl.ds(pad, count), pl.ds(pad + size, count)

        out = []
        steps = [(dz, dx) for dz in (1, -1) for dx in (1, -1)] if corner else []
        for number, (dz, dx) in enumerate(steps + [(0, 1), (0, -1), (1, 0), (-1, 0)]):
            count = corner if dz and dx else depth
            src_z, dst_z = spans(dz, deep, count)
            src_x, dst_x = spans(dx, broad, count)
            copy = pltpu.make_async_remote_copy(
                src_ref=ref.at[src_z, src_x],
                dst_ref=ref.at[dst_z, dst_x],
                send_sem=h_send.at[stage, number],
                recv_sem=h_recv.at[stage, number],
                device_id=device(dz, dx),
                device_id_type=MESH,
            )
            sends = both(has_z[dz], has_x[dx])
            arrives = both(has_z[-dz], has_x[-dx])
            out.append((sends, arrives, copy))
        return out

    started = []

    def send(ref, depth, corner, stage):
        copies = wide(ref, depth, corner, stage)
        for sends, _, copy in copies:
            pl.when(sends)(copy.start)
        started.append(copies)

    def receive():
        for _, arrives, copy in started[-1]:
            pl.when(arrives)(copy.wait_recv)

    fine, middle, coarse = FINE, scaled(FINE, 2.0), scaled(COARSE, 4.0)

    def pieces_of(ref, edge):
        _, deep, broad = size_of(ref)
        return (
            (edge, deep - 2 * edge, edge, broad - 2 * edge),
            (0, edge, 0, broad),
            (deep - edge, edge, 0, broad),
            (edge, deep - 2 * edge, 0, edge),
            (edge, deep - 2 * edge, broad - edge, edge),
        )

    pieces = [(a5, out_solution, part) for part in pieces_of(a5, 2)]
    pieces.append((fd, out_defect, (0, planes, 0, block)))

    def ends(piece, step, owner):
        src, dst, (z, deep, x, broad) = pieces[piece]
        return (
            src.at[pl.ds(z + PAD, deep), pl.ds(x + PAD, broad), step, :],
            dst.at[pl.ds(z, deep), pl.ds(snake(owner) * block + x, broad), :],
        )

    def outward(piece, peer, owner):
        src, dst = ends(piece, peer, owner)
        return pltpu.make_async_remote_copy(
            src_ref=src,
            dst_ref=dst,
            send_sem=out_send.at[piece, peer],
            recv_sem=out_recv.at[piece, owner],
            device_id={"tm": peer},
            device_id_type=MESH,
        )

    def home(piece):
        src, dst = ends(piece, me, me)
        return pltpu.make_async_copy(src, dst, out_own.at[piece])

    def ship(piece):
        for k in order:
            outward(piece, me ^ k, me).start()
        home(piece).start()

    def stages(boxes_of, works):
        for work, (ref, rings) in zip(works, boxes_of):
            over(strips(ref, *rings) if isinstance(rings, tuple) else (box(ref, rings),), work)

    def presmooth(x, right, one, two, left, gain, weights, shift, pairs):
        works = (
            starter(one, right, gain),
            sweeper(two, one, right, cond, gain, weights, shift),
            defecter(left, two, right, weights, shift, pairs),
        )
        send(right, 2, 1, x)
        stages(((one, 0), (two, -1), (left, -2)), works)
        receive()
        stages(((one, (2, 0)), (two, (1, -1)), (left, (0, -2))), works)

    own.wait()
    for k in order:
        inward(me, me ^ k, me ^ k).wait_recv()
    presmooth(0, rhs, a1, a2, rhs1, gain0, fine, 1, True)
    presmooth(1, rhs1, m1, m2, scrap, gain1, middle, 2, False)

    def restrict(z, _):
        for x in range(half_block):
            zz, xx = 2 * z + PAD, 2 * x + PAD
            quad = (scrap[zz, xx] + scrap[zz + 1, xx]) + (
                scrap[zz, xx + 1] + scrap[zz + 1, xx + 1]
            )
            rhs2[z + PAD2, x + PAD2] = 0.25 * with_partner(quad[None], 2)[0]
        return 0

    lax.fori_loop(0, half_planes, restrict, 0)
    send(rhs2, 3, 2, 2)
    start = starter(k1, rhs2, gain2)
    works = [
        sweeper(new, old, rhs2, cond2, gain2, coarse, 4)
        for new, old in ((k2, k1), (k3, k2), (k4, k3))
    ]
    stages(((k1, 0), (k2, -1)), (start, works[0]))
    receive()
    stages(((k1, (3, 0)), (k2, (2, -1)), (k3, 1), (k4, 0)), (start, *works))

    def prolong(z, x0, x1):
        for x in range(x0, x1):
            value = k4[z, x]
            for dz in range(2):
                for dx in range(2):
                    at = (2 * (z - PAD2) + dz + PAD, 2 * (x - PAD2) + dx + PAD)
                    m3[at] = m2[at] + value

    over(strips(k4, 0, -1), prolong)
    send(m3, 2, 1, 3)
    over((box(k4, -1),), prolong)
    works = (
        sweeper(m4, m3, rhs1, cond, gain1, middle, 2),
        sweeper(a3, m4, rhs1, cond, gain1, middle, 2, a2),
    )
    stages(((m4, -1), (a3, -2)), works)
    receive()
    stages(((m4, (1, -1)), (a3, (0, -2))), works)
    send(a3, 2, 1, 4)
    works = (
        sweeper(a4, a3, rhs, cond, gain0, fine, 1),
        sweeper(a5, a4, rhs, cond, gain0, fine, 1),
    )
    stages(((a4, -1), (a5, -2)), works)
    ship(0)
    receive()
    stages(((a4, (1, -1)), (a5, (0, -2))), works)
    send(a5, 1, 0, 5)
    for piece in range(1, 5):
        ship(piece)
    works = (defecter(fd, a5, rhs, fine, 1, False),)
    stages(((fd, -1),), works)
    receive()
    stages(((fd, (0, -1)),), works)
    ship(5)

    for copies in started:
        for sends, _, copy in copies:
            pl.when(sends)(copy.wait_send)
    for side, dz in ((0, 1), (1, -1)):
        pl.when(has_z[dz])(tall_copy(side, dz).wait_send)
    for k in order:
        inward(me ^ k, me, me).wait_send()
    for piece in range(6):
        home(piece).wait()
        for k in order:
            outward(piece, me ^ k, me).wait_send()
            outward(piece, me, me ^ k).wait_recv()


def fused_body(peers, slabs, source, conductivity):
    _, planes, rows, lanes = source.shape
    block = rows // peers

    def field(depth, width):
        return pltpu.VMEM((depth, width, peers, lanes), jnp.float32)

    large = field(planes + 2 * PAD, block + 2 * PAD)
    small = field(planes // 2 + 2 * PAD2, block // 2 + 2 * PAD2)
    dma = pltpu.SemaphoreType.DMA
    anywhere = pl.BlockSpec(memory_space=pl.ANY)
    shape = jax.ShapeDtypeStruct((planes, rows, lanes), jnp.float32)
    solution, final_defect = pl.pallas_call(
        functools.partial(cycle_kernel, peers, slabs),
        out_shape=(shape, shape),
        in_specs=[anywhere, anywhere],
        out_specs=(anywhere, anywhere),
        scratch_shapes=[
            large, large, small, large,
            large, small, large, large, small,
            large, large, large, large, large, large,
            large, large, large, large,
            small, small, small, small,
            pltpu.VMEM((planes, rows, lanes), jnp.float32),
            pltpu.VMEM((planes + 4 * PAD2, rows, lanes), jnp.float32),
            dma((peers,)), dma((peers,)), dma, dma((2,)),
            dma((2,)), dma((2,)),
            dma((6, 8)), dma((6, 8)),
            dma((6, peers)), dma((6, peers)), dma((6,)),
        ],
        compiler_params=pltpu.CompilerParams(
            collective_id=0, has_side_effects=True, vmem_limit_bytes=60 * 1024 * 1024
        ),
    )(source[0], conductivity)
    return (solution[None], final_defect[None])


def solution(mesh):
    peers, slabs = mesh.shape["tm"], mesh.shape["space"]

    def chosen(source, conductivity):
        steps, planes, rows, lanes = source.shape
        if fits(steps * peers, peers, slabs, planes, rows, lanes):
            return fused_body(peers, slabs, source, conductivity)
        return body(source, conductivity)

    return jax.shard_map(
        chosen,
        mesh=mesh,
        in_specs=(P("tm", "space", None, None), P("space", None, None)),
        out_specs=(P("tm", "space", None, None), P("tm", "space", None, None)),
        check_vma=False,
    )
```
